32 devices in a mesh: part: 1 (over z), data: 4 (over y), model: 8 (over x, core).
Axes of the slice: x: 4, y: 4, z: 1, core: 2. Of those that a mesh axis runs over, the one named last changes fastest.
The devices are a block of a 4x4x8 slice.
Arguments:
- x: bfloat16 [2, 64, 512, 1024], P(None, ('part', 'data'), 'model')
- lengths: int32 [2, 64], P(None, ('part', 'data'))
- norm_gain: bfloat16 [2, 1024], P(None, 'data')
- w_in: bfloat16 [2, 1024, 9216], P(None, 'data', 'model')
- w_kv: bfloat16 [2, 1024, 128], P(None, 'data')
- w_out: bfloat16 [2, 5120, 1024], P(None, 'model', 'data')
Outputs:
- output: bfloat16 [2, 64, 512, 1024], P(None, ('part', 'data'), 'model')
All inputs are finite; a program needn't handle non-finite values.
Results may differ from the reference program's by a relative error of at most 0.013324.
Values are sent between devices in bfloat16 or wider.
A program may use at most 768 MiB of HBM per device.

```python
import math
import jax
import jax.numpy as jnp
from jax import lax

N_MICRO = 2
N_LAYERS = 2
N_SEQS = 64
SEQ_LEN = 512
D_MODEL = 1024
N_HEADS = 16
HEAD_DIM = 64
D_FF = 4096
MODEL_SHARDS = 8
FF_HEAD = D_FF // N_HEADS
UNIT_IN = HEAD_DIM + 2 * FF_HEAD
UNIT_OUT = HEAD_DIM + FF_HEAD
SHARD_ROWS = (N_HEADS // MODEL_SHARDS) * UNIT_OUT
NORM_EPS = 1e-6
NEG_BIG = -1e30
Q_GAIN = math.sqrt(max(math.log(SEQ_LEN / 8.0), 1.0))


def setup_inputs(seed: int = 0, part: int = 0) -> dict:
    part_keys = jax.random.split(jax.random.fold_in(jax.random.key(seed), part), 2)
    shared_keys = jax.random.split(jax.random.key(seed + 1), 4)
    x_act = jax.random.normal(part_keys[0], (N_MICRO, N_SEQS, SEQ_LEN, D_MODEL), jnp.float32)
    seq_lens = jax.random.randint(part_keys[1], (N_MICRO, N_SEQS), SEQ_LEN // 4, SEQ_LEN + 1)
    seq_lens = seq_lens.at[0, 0].set(SEQ_LEN).at[1, 0].set(SEQ_LEN // 4)
    gain_vals = jax.random.uniform(shared_keys[0], (N_LAYERS, D_MODEL), jnp.float32, 0.5, 1.5)
    col_scale = jnp.concatenate([jnp.full((HEAD_DIM,), Q_GAIN, jnp.float32), jnp.ones((2 * FF_HEAD,), jnp.float32)]) * (D_MODEL ** -0.5)
    w_in_vals = jax.random.normal(shared_keys[1], (N_LAYERS, D_MODEL, N_HEADS, UNIT_IN), jnp.float32) * col_scale
    w_kv_vals = jax.random.normal(shared_keys[2], (N_LAYERS, D_MODEL, 2 * HEAD_DIM), jnp.float32) * (D_MODEL ** -0.5)
    row_scale = jnp.concatenate([jnp.full((HEAD_DIM,), (N_HEADS * HEAD_DIM) ** -0.5, jnp.float32), jnp.full((FF_HEAD,), D_FF ** -0.5, jnp.float32)])
    w_out_vals = jax.random.normal(shared_keys[3], (N_LAYERS, N_HEADS, UNIT_OUT, D_MODEL), jnp.float32) * row_scale[:, None]
    return {
        "x": x_act.astype(jnp.bfloat16),
        "lengths": seq_lens.astype(jnp.int32),
        "norm_gain": gain_vals.astype(jnp.bfloat16),
        "w_in": w_in_vals.reshape(N_LAYERS, D_MODEL, N_HEADS * UNIT_IN).astype(jnp.bfloat16),
        "w_kv": w_kv_vals.astype(jnp.bfloat16),
        "w_out": w_out_vals.reshape(N_LAYERS, N_HEADS * UNIT_OUT, D_MODEL).astype(jnp.bfloat16),
    }


def layer_one_seq(x_seq, seq_len, gain_vec, w_in_l, w_kv_l, w_out_l):
    x_f32 = x_seq.astype(jnp.float32)
    centered = x_f32 - jnp.mean(x_f32, axis=-1, keepdims=True)
    variance = jnp.mean(centered * centered, axis=-1, keepdims=True)
    h_act = (centered * lax.rsqrt(variance + NORM_EPS) * gain_vec.astype(jnp.float32)).astype(jnp.bfloat16)
    projected = jnp.dot(h_act, w_in_l, preferred_element_type=jnp.float32).astype(jnp.bfloat16)
    projected = projected.reshape(SEQ_LEN, N_HEADS, UNIT_IN)
    q_heads = projected[:, :, :HEAD_DIM]
    gate_act = projected[:, :, HEAD_DIM:HEAD_DIM + FF_HEAD]
    up_act = projected[:, :, HEAD_DIM + FF_HEAD:]
    kv_act = jnp.dot(h_act, w_kv_l, preferred_element_type=jnp.float32).astype(jnp.bfloat16)
    k_act = kv_act[:, :HEAD_DIM]
    v_act = kv_act[:, HEAD_DIM:]
    scores = jnp.einsum("qhc,kc->hqk", q_heads.astype(jnp.float32), k_act.astype(jnp.float32)) * (1.0 / math.sqrt(HEAD_DIM))
    positions = jnp.arange(SEQ_LEN)
    allowed = (positions[None, :] <= positions[:, None]) & (positions[None, :] < seq_len)
    scores = jnp.where(allowed[None], scores, NEG_BIG)
    attn_probs = jax.nn.softmax(scores, axis=-1).astype(jnp.bfloat16)
    attn_out = jnp.einsum("hqk,kc->qhc", attn_probs.astype(jnp.float32), v_act.astype(jnp.float32)).astype(jnp.bfloat16)
    mlp_out = (jax.nn.silu(gate_act.astype(jnp.float32)) * up_act.astype(jnp.float32)).astype(jnp.bfloat16)
    joined = jnp.concatenate([attn_out, mlp_out], axis=-1).reshape(SEQ_LEN, MODEL_SHARDS, SHARD_ROWS)
    w_groups = w_out_l.reshape(MODEL_SHARDS, SHARD_ROWS, D_MODEL)

    def add_group(running, group_pair):
        rows_in, w_rows = group_pair
        group_sum = jnp.dot(rows_in, w_rows, preferred_element_type=jnp.float32).astype(jnp.bfloat16)
        return running + group_sum.astype(jnp.float32), None

    z_sum, _ = lax.scan(add_group, jnp.zeros((SEQ_LEN, D_MODEL), jnp.float32), (jnp.swapaxes(joined, 0, 1), w_groups))
    return (x_f32 + z_sum).astype(jnp.bfloat16)


def reference(x, lengths, norm_gain, w_in, w_kv, w_out):
    seqs_x = x.reshape(N_MICRO * N_SEQS, SEQ_LEN, D_MODEL)
    seqs_len = lengths.reshape(N_MICRO * N_SEQS)

    def run_seq(seq_item):
        x_seq, seq_len = seq_item

        def one_layer(carry_x, weights):
            gain_l, w_in_l, w_kv_l, w_out_l = weights
            return layer_one_seq(carry_x, seq_len, gain_l, w_in_l, w_kv_l, w_out_l), None

        final_x, _ = lax.scan(one_layer, x_seq, (norm_gain, w_in, w_kv, w_out))
        return final_x

    y_all = lax.map(run_seq, (seqs_x, seqs_len))
    return y_all.reshape(N_MICRO, N_SEQS, SEQ_LEN, D_MODEL)
```

```python
import functools
import math
import jax
import jax.numpy as jnp
from jax import lax
from jax.experimental import pallas as pl
from jax.experimental.pallas import tpu as pltpu
from jax.sharding import PartitionSpec as P

NORM_EPS = 1e-6
NEG_BIG = -1e30
LANES = 128
SEQS_BLOCK = 8
CORES = 2
IN_SPLIT = 80
OUT_SPLIT = 320
BF16 = jnp.bfloat16
F32 = jnp.float32


def silu_mul(g, u):
    return g * (1.0 / (1.0 + jnp.exp(-g))) * u


def kernel_body(cfg, lens, x_hbm, w_in_hbm, w_out_hbm, w_kv_in, gain_in,
                y_hbm, all_in, all_out,
                w_in_buf, w_out_buf, kv_land, w_kv_all, gain_all, x_scr, h_scr, z_scr, t_scr, j_scr,
                rsem, ssem, load_sem, io_sem, own_sem):
    n_layers, n_y, n_x, t_loc, s_len, head_dim, in_loc, out_loc, n_seqs = cfg["dims"]
    copies_sem = cfg["sems"]
    d_model = x_scr.shape[1]
    rows_blk = t_scr.shape[0]
    n_blk = x_scr.shape[0] // rows_blk
    seqs_blk = rows_blk // t_loc
    f_loc = d_model // n_y
    n_units = n_x
    my_y = lax.axis_index("data")
    me = lax.axis_index("model")
    my_x, my_c = lax.div(me, CORES), lax.rem(me, CORES)
    q_off = me * t_loc
    order = [0, n_x - 1, 1] + list(range(2, n_x - 1))

    def col(j):
        return lax.rem(my_x + order[j], n_x)

    def at(dy=0, dx=0, dc=0):
        y = lax.rem(my_y + (dy % n_y), n_y)
        x = lax.rem(my_x + (dx % n_x), n_x)
        c = lax.rem(my_c + dc, CORES)
        return {"data": y, "model": x * CORES + c}

    count = [0]
    rings = []

    class Send:
        def __init__(self, dst, to, arrives, src=None):
            self.k = count[0]
            count[0] += 1
            self.dst, self.to, self.arrives, self.src = dst, to, arrives, src or dst
            rings.append(self)

        def make(self, src, dst):
            return pltpu.make_async_remote_copy(src_ref=src, dst_ref=dst, send_sem=ssem.at[self.k], recv_sem=rsem.at[self.k],
                                                device_id=at(**self.to), device_id_type=pl.DeviceIdType.MESH)

        def start(self):
            self.make(self.src(), self.dst()).start()

        def wait(self):
            self.make(self.arrives(), self.arrives()).wait_recv()

        def wait_sent(self):
            self.make(self.src(), self.dst()).wait_send()

    class Ring:
        def __init__(self, axis, piece, flip, own=None):
            n = n_y if axis == "dy" else n_x
            rank = my_y if axis == "dy" else my_x

            def p(d):
                return lambda: piece(lax.rem(rank + (d % n), n))

            self.up = Send(p(0), {axis: 1}, p(-1), own)
            self.down = Send(p(0), {axis: -1}, p(1), own)
            self.flip = flip
            self.far = Send(p(1), {axis: -1}, p(2)) if flip else Send(p(-1), {axis: 1}, p(-2))
            self.p = p

        def start(self):
            self.up.start()
            self.down.start()

        def forward(self):
            (self.down if self.flip else self.up).wait()
            self.far.start()

        def near(self):
            (self.up if self.flip else self.down).wait()

        def last(self):
            self.far.wait()

        def finish(self):
            self.near()
            self.last()

    shards = []
    for l in range(n_layers):
        kinds = []
        for kind, (own, land, split) in enumerate(((w_in_hbm, all_in, IN_SPLIT), (w_out_hbm, all_out, OUT_SPLIT))):
            rows = own.shape[1]
            odd = (l + kind) % 2 == 1
            lo, hi = pl.ds(0, split), pl.ds(split, rows - split)

            def a1(y, land=land, l=l, lo=lo):
                return land.at[l, my_c, my_x, y, lo]

            def a2(x, land=land, l=l, lo=lo):
                return land.at[l, my_c, x, :, lo]

            def b1(x, land=land, l=l, hi=hi):
                return land.at[l, my_c, x, my_y, hi]

            def b2(y, x, land=land, l=l, hi=hi):
                return land.at[l, my_c, x, y, hi]

            def own_lo(own=own, l=l, lo=lo):
                return own.at[l, lo]

            def own_hi(own=own, l=l, hi=hi):
                return own.at[l, hi]

            s = {
                "A1": Ring("dy", a1, odd, own_lo),
                "B1": Ring("dx", b1, not odd, own_hi),
                "A2": Ring("dx", a2, odd),
                "B2": [Ring("dy", (lambda y, j=j, b2=b2: b2(y, col(j))), (j + l + kind) % 2 == 0, own_hi if j == 0 else None) for j in range(n_x)],
                "D": [Send((lambda j=j, land=land, l=l: land.at[l, my_c, col(j)]), {"dc": 1},
                           (lambda j=j, land=land, l=l: land.at[l, 1 - my_c, col(j)])) for j in range(n_x)],
            }
            kinds.append(s)
        shards.append(kinds)

    kvs = []
    for l in range(n_layers):
        for b in range(n_blk):
            def kv_piece(x, c, l=l, b=b):
                return kv_land.at[l, pl.ds(b * seqs_blk, seqs_blk), pl.ds(pl.multiple_of((x * CORES + c) * t_loc, t_loc), t_loc)]

            ring = Ring("dx", (lambda x, f=kv_piece: f(x, my_c)), b % 2 == 1)
            side = []
            for d in (0, -1, 1, 2):
                def there(d=d, f=kv_piece):
                    return f(lax.rem(my_x + (d % n_x), n_x), my_c)

                def here(d=d, f=kv_piece):
                    return f(lax.rem(my_x + (d % n_x), n_x), 1 - my_c)

                side.append(Send(there, {"dc": 1}, here))
            kvs.append((ring, side))

    small = []
    for d in range(1, n_y):
        for src, dst in ((w_kv_in, w_kv_all), (gain_in, gain_all)):
            small.append(Send((lambda dst=dst: dst.at[:, my_y]), {"dy": d},
                              (lambda dst=dst, d=d: dst.at[:, lax.rem(my_y + n_y - d, n_y)]), (lambda src=src: src)))
    assert count[0] == copies_sem, count[0]

    def blk_rows(b):
        return pl.ds(pl.multiple_of(b * rows_blk, rows_blk), rows_blk)

    def load_in(l, j, slot):
        return [pltpu.make_async_copy(all_in.at[l, c, col(j)], w_in_buf.at[slot, :, :, pl.ds(c * in_loc, in_loc)], load_sem.at[slot, c]) for c in range(CORES)]

    def load_out(l, j, slot):
        return [pltpu.make_async_copy(all_out.at[l, c, col(j)], w_out_buf.at[slot, :, pl.ds(c * out_loc, out_loc)], load_sem.at[slot, 2 + c]) for c in range(CORES)]

    def norm_block(l, b):
        rows = blk_rows(b)
        gain = jnp.concatenate([gain_all[l, d, 0:1, :] for d in range(n_y)], axis=1)
        x_f32 = x_scr[rows, :].astype(F32)
        centered = x_f32 - jnp.mean(x_f32, axis=-1, keepdims=True)
        variance = jnp.mean(centered * centered, axis=-1, keepdims=True)
        h_scr[rows, :] = (centered * lax.rsqrt(variance + NORM_EPS) * gain).astype(BF16)
        kv = jnp.dot(h_scr[rows, :], w_kv_all[l].reshape(d_model, 2 * head_dim), preferred_element_type=F32).astype(BF16)
        kv_land[l, pl.ds(b * seqs_blk, seqs_blk), pl.ds(pl.multiple_of(q_off, t_loc), t_loc), :] = kv.reshape(seqs_blk, t_loc, 2 * head_dim)

    def kv_start(l, b):
        ring, side = kvs[l * n_blk + b]
        ring.start()
        side[0].start()

    def kv_forward(l, b):
        ring, side = kvs[l * n_blk + b]
        ring.forward()
        side[2 if ring.flip else 1].start()

    def kv_finish(l, b):
        ring, side = kvs[l * n_blk + b]
        ring.near()
        side[1 if ring.flip else 2].start()
        ring.last()
        side[3].start()
        for s in side:
            s.wait()

    barrier = pltpu.get_barrier_semaphore()
    peers = [{"dy": d} for d in range(1, n_y)] + [{"dx": 1}, {"dx": -1}, {"dc": 1}]
    for to in peers:
        pl.semaphore_signal(barrier, inc=1, device_id=at(**to), device_id_type=pl.DeviceIdType.MESH)

    x_in = [pltpu.make_async_copy(x_hbm.at[blk_rows(b)], x_scr.at[blk_rows(b)], io_sem.at[b]) for b in range(n_blk)]
    own = []
    for l in range(n_layers):
        own.append((w_in_hbm.at[l], w_in_buf.at[1, l, :, pl.ds(0, in_loc)], all_in.at[l, my_c, my_x, my_y], own_sem.at[l, 0]))
        own.append((w_out_hbm.at[l], w_out_buf.at[1, l, pl.ds(0, out_loc)], all_out.at[l, my_c, my_x, my_y], own_sem.at[l, 1]))
    for cp in x_in:
        cp.start()
    for src, mid, _, sem in own:
        pltpu.make_async_copy(src, mid, sem).start()
    pl.semaphore_wait(barrier, len(peers))
    for s in small:
        s.start()
    (i0, o0), (i1, o1) = shards
    i0["A1"].start()
    i0["B1"].start()
    i0["B2"][0].start()
    w_kv_all[:, my_y] = w_kv_in[...]
    gain_all[:, my_y] = gain_in[...]
    for src, mid, dst, sem in own:
        pltpu.make_async_copy(src, mid, sem).wait()
        pltpu.make_async_copy(mid, dst, sem).start()
    for s in small:
        s.wait()
    for cp in x_in:
        cp.wait()

    def first_norm(b, carry):
        norm_block(0, b)
        return carry

    lax.fori_loop(0, n_blk, first_norm, 0)
    for _, mid, dst, sem in own:
        pltpu.make_async_copy(mid, dst, sem).wait()
    for b in range(n_blk):
        kv_start(0, b)
    for ring in (o0["A1"], o0["B1"], o0["B2"][0]):
        ring.start()
    i0["A1"].forward()
    i0["B1"].forward()
    i0["B2"][0].forward()
    i0["A1"].finish()
    i0["A2"].start()
    i0["B2"][0].finish()
    i0["D"][0].start()
    i0["B1"].finish()
    for j in range(1, n_x):
        i0["B2"][j].start()
    i0["D"][0].wait()
    for cp in load_in(0, 0, 0):
        cp.start()

    def clear(b, carry):
        z_scr[blk_rows(b), :] = jnp.zeros((rows_blk, d_model), F32)
        return carry

    lax.fori_loop(0, n_blk, clear, 0)

    top, attn, late = {}, {}, {}

    def put(where, step, *acts):
        where.setdefault(step, []).extend(acts)

    def begin(cps):
        return lambda: [cp.start() for cp in cps()]

    def end(cps):
        return lambda: [cp.wait() for cp in cps()]

    steps_layer = n_units * n_blk

    def fetch(l, j, step, in_first=None):
        slot = (l * n_units + j) % 2
        i, o = shards[l]
        g = l * steps_layer + j * n_blk
        if in_first is None:
            put(late, step, i["D"][j].wait, begin(lambda: load_in(l, j, slot)))
        put(top, g, end(lambda: load_in(l, j, slot)))
        put(late, g if j == 0 and l == 0 else step, o["D"][j].wait, begin(lambda: load_out(l, j, slot)))
        put(late, g, end(lambda: load_out(l, j, slot)))

    for b in range(n_blk):
        put(attn, 0, lambda b=b: kv_forward(0, b))
    for b in range(n_blk):
        put(attn, b, lambda b=b: kv_finish(0, b))
    put(late, 0, o0["A1"].forward, o0["B1"].forward, o0["B2"][0].forward, o0["A1"].finish, o0["A2"].start, o0["B2"][0].finish, o0["D"][0].start)
    fetch(0, 0, 0, in_first=True)
    put(attn, 1, o0["B1"].finish, *[o0["B2"][j].start for j in range(1, n_x)])
    put(top, 2, i0["A2"].forward, i0["B2"][1].forward)
    put(top, 3, i0["B2"][2].forward, i0["B2"][1].finish)
    a2_first, a2_second = ((i0["A2"].down, i0["A2"].up) if i0["A2"].flip else (i0["A2"].up, i0["A2"].down))
    put(top, 3, i0["A2"].near, i0["D"][1].start, i0["B2"][2].finish, i0["D"][2].start)
    put(late, 3, i0["B2"][3].forward, o0["A2"].forward, o0["B2"][1].forward, o0["B2"][2].forward, o0["B2"][1].finish, o0["A2"].near, o0["D"][1].start)
    fetch(0, 1, 3)
    put(attn, 5, o0["B2"][2].finish, o0["D"][2].start, o0["B2"][3].forward)
    put(late, 6, i0["A2"].last, i0["B2"][3].finish, i0["D"][3].start)
    fetch(0, 2, 7)
    put(late, 8, o0["A2"].last, o0["B2"][3].finish, o0["D"][3].start)
    fetch(0, 3, 11)
    put(top, 7, *[r.start for r in (i1["A1"], i1["B1"], i1["B2"][0], o1["A1"], o1["B1"], o1["B2"][0])])
    put(attn, 9, i1["A1"].forward, i1["B1"].forward, i1["B2"][0].forward)
    put(top, 10, o1["A1"].forward, o1["B1"].forward, o1["B2"][0].forward, i1["A1"].finish, i1["A2"].start)
    put(attn, 10, i1["B2"][0].finish, i1["D"][0].start, i1["B1"].finish, *[i1["B2"][j].start for j in range(1, n_x)])
    put(top, 11, o1["A1"].finish, o1["A2"].start, o1["B2"][0].finish, o1["D"][0].start, o1["B1"].finish, *[o1["B2"][j].start for j in range(1, n_x)])
    put(top, 13, i1["A2"].forward, i1["B2"][1].forward, i1["B2"][2].forward)
    put(top, 14, i1["A2"].near, i1["B2"][1].finish, i1["D"][1].start, i1["B2"][2].finish, i1["D"][2].start)
    fetch(1, 0, 15)
    put(top, 15, o1["A2"].forward, i1["B2"][3].forward, o1["B2"][1].forward, o1["B2"][2].forward)
    put(top, 17, o1["A2"].near, o1["B2"][1].finish, o1["D"][1].start, o1["B2"][2].finish, o1["D"][2].start, o1["B2"][3].forward)
    put(top, 18, i1["A2"].last, i1["B2"][3].finish, i1["D"][3].start)
    fetch(1, 1, 19)
    put(top, 20, o1["A2"].last, o1["B2"][3].finish, o1["D"][3].start)
    fetch(1, 2, 23)
    fetch(1, 3, 27)
    for b in range(n_blk):
        put(attn, steps_layer - n_blk + b + 1, lambda b=b: kv_forward(1, b))
        put(attn, steps_layer + b, lambda b=b: kv_finish(1, b))

    def run(where, g):
        for step, acts in sorted(where.items()):
            @pl.when(g == step)
            def _(acts=acts):
                for act in acts:
                    act()

    n_in = w_in_buf.shape[3]
    tiles_in, tiles_out = in_loc // LANES, out_loc // LANES
    low = lax.broadcasted_iota(jnp.int32, (rows_blk, LANES), 1) < head_dim
    low_q = lax.broadcasted_iota(jnp.int32, (t_loc, LANES), 1) < head_dim
    row_pos = q_off + lax.broadcasted_iota(jnp.int32, (t_loc, 1), 0)
    key_pos = lax.broadcasted_iota(jnp.int32, (t_loc, s_len), 1)
    scale = 1.0 / math.sqrt(head_dim)

    def step(g, carry):
        l = lax.div(g, steps_layer)
        u = lax.rem(lax.div(g, n_blk), n_units)
        b = lax.rem(g, n_blk)
        slot = lax.rem(lax.div(g, n_blk), 2)
        rows = blk_rows(b)
        run(top, g)
        h_blk = h_scr[rows, :]
        for c in range(0, n_in, 256):
            w = w_in_buf[slot, :, :, c:c + 256].reshape(d_model, 256)
            t_scr[:, c:c + 256] = jnp.dot(h_blk, w, preferred_element_type=F32).astype(BF16)

        def tile(i):
            return t_scr[:, i * LANES:(i + 1) * LANES].astype(F32)

        for c in range(CORES):
            ti, tj = c * tiles_in, c * tiles_out
            for gate, up, out in ((1, 3, 1), (5, 7, 3), (6, 8, 4)):
                j_scr[:, (tj + out) * LANES:(tj + out + 1) * LANES] = silu_mul(tile(ti + gate), tile(ti + up)).astype(BF16)
            t2 = tile(ti + 2)
            mixed = silu_mul(jnp.where(low, t2, tile(ti)), jnp.where(low, tile(ti + 4), t2)).astype(BF16)
            j_scr[:, tj * LANES:(tj + 1) * LANES] = mixed
            j_scr[:, (tj + 2) * LANES:(tj + 3) * LANES] = mixed
        run(attn, g)

        def one_seq(i, c_seq):
            r = pl.ds(pl.multiple_of(i * t_loc, t_loc), t_loc)
            heads = []
            for c in range(CORES):
                ti = c * tiles_in
                q0 = t_scr[r, ti * LANES:(ti + 1) * LANES].astype(F32)
                q1 = pltpu.roll(t_scr[r, (ti + 4) * LANES:(ti + 5) * LANES].astype(F32), head_dim, 1)
                heads += [jnp.where(low_q, q, 0.0).astype(BF16) for q in (q0, q1)]
            seq = b * seqs_blk + i
            kv = kv_land[l, seq]
            scores = lax.dot_general(jnp.concatenate(heads, axis=0), kv, (((1,), (1,)), ((), ())), preferred_element_type=F32)
            allowed = key_pos < jnp.minimum(row_pos + 1, lens[seq])
            probs = []
            for k in range(len(heads)):
                s = jnp.where(allowed, scores[k * t_loc:(k + 1) * t_loc] * scale, NEG_BIG)
                e = jnp.exp(s - jnp.max(s, axis=-1, keepdims=True))
                probs.append((e * (1.0 / jnp.sum(e, axis=-1, keepdims=True))).astype(BF16))
            o = jnp.dot(jnp.concatenate(probs, axis=0), kv, preferred_element_type=F32)
            for c in range(CORES):
                tj = c * tiles_out
                c0, c2 = slice(tj * LANES, (tj + 1) * LANES), slice((tj + 2) * LANES, (tj + 3) * LANES)
                o_a = pltpu.roll(o[2 * c * t_loc:(2 * c + 1) * t_loc], head_dim, 1)
                o_b = o[(2 * c + 1) * t_loc:(2 * c + 2) * t_loc]
                j_scr[r, c0] = jnp.where(low_q, o_a, j_scr[r, c0].astype(F32)).astype(BF16)
                j_scr[r, c2] = jnp.where(low_q, j_scr[r, c2].astype(F32), o_b).astype(BF16)
            return c_seq

        lax.fori_loop(0, seqs_blk, one_seq, 0)
        run(late, g)
        for n in range(n_y):
            cols = slice(n * f_loc, (n + 1) * f_loc)
            total = z_scr[rows, cols]
            for c in range(CORES):
                part = slice(c * out_loc, (c + 1) * out_loc)
                z_j = jnp.dot(j_scr[:, part], w_out_buf[slot, n, part, :], preferred_element_type=F32)
                total = total + z_j.astype(BF16).astype(F32)
            z_scr[rows, cols] = total

        @pl.when(u == n_units - 1)
        def _():
            x_scr[rows, :] = (x_scr[rows, :].astype(F32) + z_scr[rows, :]).astype(BF16)
            z_scr[rows, :] = jnp.zeros((rows_blk, d_model), F32)

            @pl.when(l < n_layers - 1)
            def _():
                norm_block(1, b)

        for k in range(n_blk):
            @pl.when(g == steps_layer - n_blk + k)
            def _(k=k):
                kv_start(1, k)

            @pl.when(g == n_layers * steps_layer - n_blk + k)
            def _(k=k):
                pltpu.make_async_copy(x_scr.at[blk_rows(k)], y_hbm.at[blk_rows(k)], io_sem.at[k]).start()
        return carry

    lax.fori_loop(0, n_layers * steps_layer, step, 0)
    for s in rings:
        s.wait_sent()
    for b in range(n_blk):
        pltpu.make_async_copy(x_scr.at[blk_rows(b)], y_hbm.at[blk_rows(b)], io_sem.at[b]).wait()


def count_copies(n_layers, n_x, n_y, n_blk):
    per_kind = 3 * (3 + n_x) + n_x
    return n_layers * 2 * per_kind + n_layers * n_blk * 7 + 2 * (n_y - 1)


def run_layers(mesh, x_act, lens, w_in, w_out, w_kv, gain, t_loc):
    n_tok, d_model = x_act.shape
    n_layers, f_loc, in_loc = w_in.shape
    out_loc = w_out.shape[1]
    n_y, n_model = mesh.shape["data"], mesh.shape["model"]
    n_x = n_model // CORES
    head_dim = w_kv.shape[2] // 2
    n_seqs = n_tok // t_loc
    s_len = t_loc * n_model
    rows_blk = SEQS_BLOCK * t_loc
    n_blk = n_tok // rows_blk
    n_sem = count_copies(n_layers, n_x, n_y, n_blk)
    cfg = {"dims": (n_layers, n_y, n_x, t_loc, s_len, head_dim, in_loc, out_loc, n_seqs), "sems": n_sem}
    vmem = pl.BlockSpec(memory_space=pltpu.VMEM)
    hbm = pl.BlockSpec(memory_space=pl.ANY)
    gain8 = jnp.broadcast_to(gain.astype(F32)[:, None, :], (n_layers, 8, f_loc))
    return pl.pallas_call(
        functools.partial(kernel_body, cfg),
        out_shape=(
            jax.ShapeDtypeStruct((n_tok, d_model), BF16),
            jax.ShapeDtypeStruct((n_layers, CORES, n_x, n_y, f_loc, in_loc), BF16),
            jax.ShapeDtypeStruct((n_layers, CORES, n_x, n_y, out_loc, f_loc), BF16),
        ),
        in_specs=[pl.BlockSpec(memory_space=pltpu.SMEM), hbm, hbm, hbm, vmem, vmem],
        out_specs=(hbm, hbm, hbm),
        scratch_shapes=[
            pltpu.VMEM((2, n_y, f_loc, CORES * in_loc), BF16),
            pltpu.VMEM((2, n_y, CORES * out_loc, f_loc), BF16),
            pltpu.VMEM((n_layers, n_seqs, s_len, 2 * head_dim), BF16),
            pltpu.VMEM((n_layers, n_y, f_loc, 2 * head_dim), BF16),
            pltpu.VMEM((n_layers, n_y, 8, f_loc), F32),
            pltpu.VMEM((n_tok, d_model), BF16),
            pltpu.VMEM((n_tok, d_model), BF16),
            pltpu.VMEM((n_tok, d_model), F32),
            pltpu.VMEM((rows_blk, CORES * in_loc), BF16),
            pltpu.VMEM((rows_blk, CORES * out_loc), BF16),
            pltpu.SemaphoreType.DMA((n_sem,)),
            pltpu.SemaphoreType.DMA((n_sem,)),
            pltpu.SemaphoreType.DMA((2, 4)),
            pltpu.SemaphoreType.DMA((n_blk,)),
            pltpu.SemaphoreType.DMA((n_layers, 2)),
        ],
        compiler_params=pltpu.CompilerParams(collective_id=0, has_side_effects=True, vmem_limit_bytes=67043328 - 1024 * 1024),
        name="layers",
    )(lens, x_act, w_in, w_out, w_kv, gain8)[0]


def solution(mesh):
    act_spec = P(None, ("part", "data"), "model", None)

    def local_fn(x_blk, len_blk, gain_blk, w_in_blk, w_kv_blk, w_out_blk):
        n_micro, n_seqs, t_loc, d_model = x_blk.shape
        x_act = x_blk.reshape(n_micro * n_seqs * t_loc, d_model)
        y = run_layers(mesh, x_act, len_blk.reshape(-1), w_in_blk, w_out_blk, w_kv_blk, gain_blk, t_loc)
        return y.reshape(x_blk.shape)

    return jax.shard_map(
        local_fn,
        mesh=mesh,
        in_specs=(act_spec, P(None, ("part", "data")), P(None, "data"), P(None, "data", "model"), P(None, "data", None), P(None, "model", "data")),
        out_specs=act_spec,
        check_vma=False,
    )
```

```python
import functools
import math
import jax
import jax.numpy as jnp
from jax import lax
from jax.experimental import pallas as pl
from jax.experimental.pallas import tpu as pltpu
from jax.sharding import PartitionSpec as P

NORM_EPS = 1e-6
NEG_BIG = -1e30
LANES = 128
SEQS_BLOCK = 8
SOFT_ROWS = 16
CORES = 2
IN_SPLIT = 80
OUT_SPLIT = 256
BF16 = jnp.bfloat16
F32 = jnp.float32
LINK_RATE, SIDE_RATE = 36e3, 300e3
STEP_TIMES = (2.4, 2.3, 1.6)
BACKLOG = 4.0
RING_WAIT, SIDE_WAIT = 3.0, 2.0


def make_actions(n_layers, n_units, n_blk):
    copies, actions = {}, []
    for l in range(n_layers):
        for k in range(2):
            first = (l + k) % 2 == 1
            rings = [(("A1", l, k), "y", "lo", first), (("B1", l, k), "x", "hi", not first), (("A2", l, k), "x", "lo4", first)]
            rings += [(("B2", l, k, j), "y", "hi", (j + l + k) % 2 == 0) for j in range(n_units)]
            for name, axis, size, flip in rings:
                copies[name + ("up",)] = (axis + "+", (size, k))
                copies[name + ("down",)] = (axis + "-", (size, k))
                copies[name + ("far",)] = (axis + ("-" if flip else "+"), (size, k))
            for j in range(n_units):
                copies[("D", l, k, j)] = ("c", ("all", k))

            def near(name, flip):
                return name + ("down" if flip else "up",)

            def pr(j, extra=0):
                return (l * n_units + j) * 10 + 3 * k + extra

            a1, b1, a2 = ("A1", l, k), ("B1", l, k), ("A2", l, k)
            whole = [a1 + (d,) for d in ("up", "down", "far")]
            for d in ("up", "down"):
                actions.append(([a1 + (d,)], [], pr(0)))
                actions.append(([("B2", l, k, 0, d)], [], pr(0)))
                actions.append(([b1 + (d,)], [], pr(1, -4)))
                actions.append(([a2 + (d,)], whole, pr(1 if d == "up" else 2)))
                for j in range(1, n_units):
                    actions.append(([("B2", l, k, j, d)], [b1 + (("up", "down", "far")[j - 1],)], pr(j)))
            for name, _, _, flip in rings:
                j = {"A1": 0, "B1": n_units - 1, "A2": n_units - 1}.get(name[0], name[-1])
                actions.append(([name + ("far",)], [near(name, flip)], pr(j, -1)))
            for j in range(n_units):
                part = whole if j == 0 else [a2 + (("up", "down", "far")[j - 1],)]
                actions.append(([("D", l, k, j)], part + [("B2", l, k, j, d) for d in ("up", "down", "far")], pr(j, -2)))
    for l in range(n_layers):
        for b in range(n_blk):
            name, flip = ("kv", l, b), b % 2 == 1
            p = l * n_units * 10 + 1 - (5 if l else 0)
            copies[name + ("up",)] = ("x+", ("kv", 0))
            copies[name + ("down",)] = ("x-", ("kv", 0))
            copies[name + ("far",)] = ("x-" if flip else "x+", ("kv", 0))
            for i in range(4):
                copies[("kvs", l, b, i)] = ("c", ("kv", 0))
            actions.append(([name + ("far",)], [name + ("down" if flip else "up",)], p))
            for i, d in enumerate(("up", "down", "far")):
                actions.append(([("kvs", l, b, i + 1)], [name + (d,)], p))
    return copies, actions


def make_plan(n_layers, n_units, n_blk, sizes):
    copies, actions = make_actions(n_layers, n_units, n_blk)
    layer = n_units * n_blk
    queue, done, waited, todo = {}, {}, set(), sorted(actions, key=lambda a: a[2])
    owner = {key: a for a in actions for key in a[0]}
    plan, loaded, now = {}, {}, [0.0]

    def start(key, out):
        link, size = copies[key]
        begin = max(now[0], queue.get(link, 0.0))
        queue[link] = begin + sizes[size] / (SIDE_RATE if link == "c" else LINK_RATE)
        done[key] = queue[link] + (SIDE_WAIT if link == "c" else RING_WAIT)
        out.append(("start", key))

    def wait(key, out):
        if key not in waited:
            now[0] = max(now[0], done[key])
            waited.add(key)
            out.append(("wait", key))

    def sweep(out, must=()):
        moved = True
        while moved:
            moved = False
            for act in list(todo):
                keys, needs, _ = act
                if any(n not in done or (n not in waited and done[n] > now[0]) for n in needs):
                    continue
                if not any(k in must for k in keys) and any(queue.get(copies[k][0], 0.0) > now[0] + BACKLOG for k in keys):
                    continue
                for n in needs:
                    wait(n, out)
                for k in keys:
                    start(k, out)
                todo.remove(act)
                moved = True

    def need(keys, out):
        must, stack = set(), list(keys)
        while stack:
            k = stack.pop()
            if k not in must:
                must.add(k)
                if k in owner:
                    stack += owner[k][1]
        while True:
            sweep(out, must)
            left = [k for k in must if k in done and k not in waited]
            if all(k in waited for k in keys):
                return
            wait(min(left, key=lambda k: done[k]), out)

    def load(l, k, j, out):
        if (l, k, j) not in loaded:
            need([("D", l, k, j)], out)
            out.append(("load", l, k, j))
            loaded[(l, k, j)] = now[0] + 2.5

    def whole(l, k, j):
        ring = ("A1", l, k) if j == 0 else None
        keys = [ring + (d,) for d in ("up", "down", "far")] if ring else [("A2", l, k, ("up", "down", "far")[j - 1])]
        return keys + [("B2", l, k, j, d) for d in ("up", "down", "far")] + [("D", l, k, j)]

    def early(at, out):
        for l in range(n_layers):
            for j in range(n_units):
                for k in range(2):
                    u = l * n_units + j
                    if (l, k, j) in loaded or at < (u - 1) * n_blk:
                        continue
                    if all(q in done and done[q] <= now[0] for q in whole(l, k, j)):
                        need(whole(l, k, j), out)
                        load(l, k, j, out)

    now[0] = 3.0
    plan["entry"] = []
    sweep(plan["entry"])
    now[0] = 12.0
    out = plan["begin"] = []
    for b in range(n_blk):
        for key in (("kv", 0, b, "up"), ("kv", 0, b, "down"), ("kvs", 0, b, 0)):
            start(key, out)
    need(whole(0, 0, 0), out)
    load(0, 0, 0, out)
    for g in range(n_layers * layer):
        l, j, b = g // layer, g // n_blk % n_units, g % n_blk
        out = plan["top", g] = []
        sweep(out)
        early(g, out)
        if b == 0:
            need(whole(l, 0, j), out)
            load(l, 0, j, out)
            now[0] = max(now[0], loaded[(l, 0, j)])
            out.append(("loaded", l, 0, j))
        now[0] += STEP_TIMES[0]
        out = plan["attn", g] = []
        sweep(out)
        early(g, out)
        if j == 0:
            need([("kv", l, b, d) for d in ("up", "down", "far")] + [("kvs", l, b, i) for i in range(4)], out)
        now[0] += STEP_TIMES[1]
        out = plan["late", g] = []
        sweep(out)
        early(g, out)
        if b == 0:
            need(whole(l, 1, j), out)
            load(l, 1, j, out)
            now[0] = max(now[0], loaded[(l, 1, j)])
            out.append(("loaded", l, 1, j))
        now[0] += STEP_TIMES[2]
        if j == n_units - 1:
            now[0] += 0.9
            if l + 1 < n_layers:
                out = plan["end", g] = []
                for key in (("kv", l + 1, b, "up"), ("kv", l + 1, b, "down"), ("kvs", l + 1, b, 0)):
                    start(key, out)
    assert not todo and waited == set(copies)
    return list(copies), plan, now[0]


def silu_mul(g, u):
    return g * (1.0 / (1.0 + jnp.exp(-g))) * u


def kernel_body(cfg, lens, x_hbm, w_in_hbm, w_out_hbm, w_kv_in, gain_in,
                y_hbm, all_in, all_out,
                w_in_buf, w_out_buf, kv_land, w_kv_all, gain_all, x_scr, h_scr, z_scr, t_scr, j_scr, s_a, s_b, p_a, p_b,
                rsem, ssem, load_sem, io_sem, own_sem):
    n_layers, n_y, n_x, t_loc, s_len, head_dim, in_loc, out_loc, n_seqs = cfg["dims"]
    keys, plan = cfg["plan"]
    d_model = x_scr.shape[1]
    rows_blk = t_scr.shape[0]
    n_blk = x_scr.shape[0] // rows_blk
    seqs_blk = rows_blk // t_loc
    f_loc = d_model // n_y
    n_units = n_x
    my_y = lax.axis_index("data")
    me = lax.axis_index("model")
    my_x, my_c = lax.div(me, CORES), lax.rem(me, CORES)
    q_off = me * t_loc
    order = [0, n_x - 1, 1] + list(range(2, n_x - 1))

    def col(j):
        return lax.rem(my_x + order[j], n_x)

    def at(dy=0, dx=0, dc=0):
        y = lax.rem(my_y + (dy % n_y), n_y)
        x = lax.rem(my_x + (dx % n_x), n_x)
        c = lax.rem(my_c + dc, CORES)
        return {"data": y, "model": x * CORES + c}

    sends = {}

    class Send:
        def __init__(self, key, dst, to, arrives, src=None):
            self.k = len(sends)
            self.dst, self.to, self.arrives, self.src = dst, to, arrives, src or dst
            sends[key] = self

        def make(self, src, dst):
            return pltpu.make_async_remote_copy(src_ref=src, dst_ref=dst, send_sem=ssem.at[self.k], recv_sem=rsem.at[self.k],
                                                device_id=at(**self.to), device_id_type=pl.DeviceIdType.MESH)

        def start(self):
            self.make(self.src(), self.dst()).start()

        def wait(self):
            self.make(self.arrives(), self.arrives()).wait_recv()

        def wait_sent(self):
            self.make(self.src(), self.dst()).wait_send()

    def ring(key, axis, piece, flip, own=None):
        n = n_y if axis == "dy" else n_x
        rank = my_y if axis == "dy" else my_x

        def p(d):
            return lambda: piece(lax.rem(rank + (d % n), n))

        Send(key + ("up",), p(0), {axis: 1}, p(-1), own)
        Send(key + ("down",), p(0), {axis: -1}, p(1), own)
        if flip:
            Send(key + ("far",), p(1), {axis: -1}, p(2))
        else:
            Send(key + ("far",), p(-1), {axis: 1}, p(-2))

    for l in range(n_layers):
        for k, (own, land, split) in enumerate(((w_in_hbm, all_in, IN_SPLIT), (w_out_hbm, all_out, OUT_SPLIT))):
            odd = (l + k) % 2 == 1
            lo, hi = pl.ds(0, split), pl.ds(split, own.shape[1] - split)

            def a1(y, land=land, l=l, lo=lo):
                return land.at[l, my_c, my_x, y, lo]

            def a2(x, land=land, l=l, lo=lo):
                return land.at[l, my_c, x, :, lo]

            def b1(x, land=land, l=l, hi=hi):
                return land.at[l, my_c, x, my_y, hi]

            def own_lo(own=own, l=l, lo=lo):
                return own.at[l, lo]

            def own_hi(own=own, l=l, hi=hi):
                return own.at[l, hi]

            ring(("A1", l, k), "dy", a1, odd, own_lo)
            ring(("B1", l, k), "dx", b1, not odd, own_hi)
            ring(("A2", l, k), "dx", a2, odd)
            for j in range(n_units):
                def b2(y, land=land, l=l, hi=hi, j=j):
                    return land.at[l, my_c, col(j), y, hi]

                def unit_of(c, land=land, l=l, j=j):
                    return land.at[l, c, col(j)]

                ring(("B2", l, k, j), "dy", b2, (j + l + k) % 2 == 0, own_hi if j == 0 else None)
                Send(("D", l, k, j), (lambda f=unit_of: f(my_c)), {"dc": 1}, (lambda f=unit_of: f(1 - my_c)))

    for l in range(n_layers):
        for b in range(n_blk):
            def kv_piece(x, c, l=l, b=b):
                return kv_land.at[l, pl.ds(b * seqs_blk, seqs_blk), pl.ds(pl.multiple_of((x * CORES + c) * t_loc, t_loc), t_loc)]

            ring(("kv", l, b), "dx", (lambda x, f=kv_piece: f(x, my_c)), b % 2 == 1)
            for i, d in enumerate((0, -1, 1, 2)):
                def side(c, d=d, f=kv_piece):
                    return f(lax.rem(my_x + (d % n_x), n_x), c)

                Send(("kvs", l, b, i), (lambda f=side: f(my_c)), {"dc": 1}, (lambda f=side: f(1 - my_c)))
    assert set(sends) == set(keys)
    small = []
    for d in range(1, n_y):
        for name, src, dst in (("kv", w_kv_in, w_kv_all), ("gain", gain_in, gain_all)):
            small.append(Send((name, d), (lambda dst=dst: dst.at[:, my_y]), {"dy": d},
                              (lambda dst=dst, d=d: dst.at[:, lax.rem(my_y + n_y - d, n_y)]), (lambda src=src: src)))
    small = [sends[k] for k in sends if k not in set(keys)]

    def blk_rows(b):
        return pl.ds(pl.multiple_of(b * rows_blk, rows_blk), rows_blk)

    def load_in(l, j, slot):
        return [pltpu.make_async_copy(all_in.at[l, c, col(j)], w_in_buf.at[slot, :, :, pl.ds(c * in_loc, in_loc)], load_sem.at[slot, c]) for c in range(CORES)]

    def load_out(l, j, slot):
        return [pltpu.make_async_copy(all_out.at[l, c, col(j)], w_out_buf.at[slot, :, pl.ds(c * out_loc, out_loc)], load_sem.at[slot, 2 + c]) for c in range(CORES)]

    def norm_block(l, b):
        rows = blk_rows(b)
        gain = jnp.concatenate([gain_all[l, d, 0:1, :] for d in range(n_y)], axis=1)
        x_f32 = x_scr[rows, :].astype(F32)
        centered = x_f32 - jnp.mean(x_f32, axis=-1, keepdims=True)
        variance = jnp.mean(centered * centered, axis=-1, keepdims=True)
        h_scr[rows, :] = (centered * lax.rsqrt(variance + NORM_EPS) * gain).astype(BF16)
        kv = jnp.dot(h_scr[rows, :], w_kv_all[l].reshape(d_model, 2 * head_dim), preferred_element_type=F32).astype(BF16)
        kv_land[l, pl.ds(b * seqs_blk, seqs_blk), pl.ds(pl.multiple_of(q_off, t_loc), t_loc), :] = kv.reshape(seqs_blk, t_loc, 2 * head_dim)

    def perform(ops):
        for op, *what in ops:
            if op == "start":
                sends[what[0]].start()
            elif op == "wait":
                sends[what[0]].wait()
            else:
                l, k, j = what
                for cp in (load_out if k else load_in)(l, j, (l * n_units + j) % 2):
                    cp.start() if op == "load" else cp.wait()

    barrier = pltpu.get_barrier_semaphore()
    peers = [{"dy": d} for d in range(1, n_y)] + [{"dx": 1}, {"dx": -1}, {"dc": 1}]
    for to in peers:
        pl.semaphore_signal(barrier, inc=1, device_id=at(**to), device_id_type=pl.DeviceIdType.MESH)

    x_in = [pltpu.make_async_copy(x_hbm.at[blk_rows(b)], x_scr.at[blk_rows(b)], io_sem.at[b]) for b in range(n_blk)]
    own = []
    for l in range(n_layers):
        own.append((w_in_hbm.at[l], w_in_buf.at[1, l, :, pl.ds(0, in_loc)], all_in.at[l, my_c, my_x, my_y], own_sem.at[l, 0]))
        own.append((w_out_hbm.at[l], w_out_buf.at[1, l, pl.ds(0, out_loc)], all_out.at[l, my_c, my_x, my_y], own_sem.at[l, 1]))
    for cp in x_in:
        cp.start()
    for src, mid, _, sem in own:
        pltpu.make_async_copy(src, mid, sem).start()
    pl.semaphore_wait(barrier, len(peers))
    for s in small:
        s.start()
    perform(plan["entry"])
    w_kv_all[:, my_y] = w_kv_in[...]
    gain_all[:, my_y] = gain_in[...]
    for src, mid, dst, sem in own:
        pltpu.make_async_copy(src, mid, sem).wait()
        pltpu.make_async_copy(mid, dst, sem).start()
    for s in small:
        s.wait()
    for cp in x_in:
        cp.wait()

    def first_norm(b, carry):
        norm_block(0, b)
        return carry

    lax.fori_loop(0, n_blk, first_norm, 0)
    for _, mid, dst, sem in own:
        pltpu.make_async_copy(mid, dst, sem).wait()
    perform(plan["begin"])

    def clear(b, carry):
        z_scr[blk_rows(b), :] = jnp.zeros((rows_blk, d_model), F32)
        return carry

    lax.fori_loop(0, n_blk, clear, 0)

    steps_layer = n_units * n_blk

    def run(point, g):
        for step in range(n_layers * steps_layer):
            if plan.get((point, step)):
                @pl.when(g == step)
                def _(step=step):
                    perform(plan[point, step])

    n_in = w_in_buf.shape[3]
    tiles_in, tiles_out = in_loc // LANES, out_loc // LANES
    low = lax.broadcasted_iota(jnp.int32, (rows_blk, LANES), 1) < head_dim
    low_q = lax.broadcasted_iota(jnp.int32, (t_loc, LANES), 1) < head_dim
    row_pos = q_off + lax.broadcasted_iota(jnp.int32, (SOFT_ROWS, 1), 0)
    key_pos = lax.broadcasted_iota(jnp.int32, (SOFT_ROWS, s_len), 1)
    scale = 1.0 / math.sqrt(head_dim)
    s_scr, p_scr = (s_a, s_b), (p_a, p_b)

    def step(g, carry):
        l = lax.div(g, steps_layer)
        u = lax.rem(lax.div(g, n_blk), n_units)
        b = lax.rem(g, n_blk)
        slot = lax.rem(lax.div(g, n_blk), 2)
        rows = blk_rows(b)
        run("top", g)
        h_blk = h_scr[rows, :]
        for c in range(0, n_in, 256):
            w = w_in_buf[slot, :, :, c:c + 256].reshape(d_model, 256)
            t_scr[:, c:c + 256] = jnp.dot(h_blk, w, preferred_element_type=F32).astype(BF16)

        def tile(i):
            return t_scr[:, i * LANES:(i + 1) * LANES].astype(F32)

        for c in range(CORES):
            ti, tj = c * tiles_in, c * tiles_out
            for gate, up, out in ((1, 3, 1), (5, 7, 3), (6, 8, 4)):
                j_scr[:, (tj + out) * LANES:(tj + out + 1) * LANES] = silu_mul(tile(ti + gate), tile(ti + up)).astype(BF16)
            t2 = tile(ti + 2)
            mixed = silu_mul(jnp.where(low, t2, tile(ti)), jnp.where(low, tile(ti + 4), t2)).astype(BF16)
            j_scr[:, tj * LANES:(tj + 1) * LANES] = mixed
            j_scr[:, (tj + 2) * LANES:(tj + 3) * LANES] = mixed
        run("attn", g)

        def score_seq(i):
            r = slice(i * t_loc, (i + 1) * t_loc)
            heads = []
            for c in range(CORES):
                ti = c * tiles_in
                q0 = t_scr[r, ti * LANES:(ti + 1) * LANES].astype(F32)
                q1 = pltpu.roll(t_scr[r, (ti + 4) * LANES:(ti + 5) * LANES].astype(F32), head_dim, 1)
                heads += [jnp.where(low_q, q, 0.0).astype(BF16) for q in (q0, q1)]
            kv = kv_land[l, b * seqs_blk + i]
            s_scr[i % 2][...] = lax.dot_general(jnp.concatenate(heads, axis=0), kv, (((1,), (1,)), ((), ())), preferred_element_type=F32)

        def soft_seq(i):
            for r in range(0, t_loc, SOFT_ROWS):
                bound = jnp.minimum(row_pos + (r + 1), lens[b * seqs_blk + i])
                allowed = key_pos < bound
                for k in range(2 * CORES):
                    part = slice(k * t_loc + r, k * t_loc + r + SOFT_ROWS)
                    s = jnp.where(allowed, s_scr[i % 2][part], NEG_BIG)
                    e = jnp.exp2((s - jnp.max(s, axis=-1, keepdims=True)) * (scale * math.log2(math.e)))
                    p_scr[i % 2][part] = (e * (1.0 / jnp.sum(e, axis=-1, keepdims=True))).astype(BF16)

        def value_seq(i):
            r = slice(i * t_loc, (i + 1) * t_loc)
            o = jnp.dot(p_scr[i % 2][...], kv_land[l, b * seqs_blk + i], preferred_element_type=F32)
            for c in range(CORES):
                tj = c * tiles_out
                c0, c2 = slice(tj * LANES, (tj + 1) * LANES), slice((tj + 2) * LANES, (tj + 3) * LANES)
                o_a = pltpu.roll(o[2 * c * t_loc:(2 * c + 1) * t_loc], head_dim, 1)
                o_b = o[(2 * c + 1) * t_loc:(2 * c + 2) * t_loc]
                j_scr[r, c0] = jnp.where(low_q, o_a, j_scr[r, c0].astype(F32)).astype(BF16)
                j_scr[r, c2] = jnp.where(low_q, j_scr[r, c2].astype(F32), o_b).astype(BF16)

        for i in range(seqs_blk + 2):
            if i < seqs_blk:
                score_seq(i)
            if 0 <= i - 2:
                value_seq(i - 2)
            if 0 <= i - 1 < seqs_blk:
                soft_seq(i - 1)
        run("late", g)
        for n in range(n_y):
            cols = slice(n * f_loc, (n + 1) * f_loc)
            total = z_scr[rows, cols]
            for c in range(CORES):
                part = slice(c * out_loc, (c + 1) * out_loc)
                z_j = jnp.dot(j_scr[:, part], w_out_buf[slot, n, part, :], preferred_element_type=F32)
                total = total + z_j.astype(BF16).astype(F32)
            z_scr[rows, cols] = total

        @pl.when(u == n_units - 1)
        def _():
            x_scr[rows, :] = (x_scr[rows, :].astype(F32) + z_scr[rows, :]).astype(BF16)
            z_scr[rows, :] = jnp.zeros((rows_blk, d_model), F32)

            @pl.when(l < n_layers - 1)
            def _():
                norm_block(1, b)

        run("end", g)
        for k in range(n_blk):
            @pl.when(g == n_layers * steps_layer - n_blk + k)
            def _(k=k):
                pltpu.make_async_copy(x_scr.at[blk_rows(k)], y_hbm.at[blk_rows(k)], io_sem.at[k]).start()
        return carry

    lax.fori_loop(0, n_layers * steps_layer, step, 0)
    for s in sends.values():
        s.wait_sent()
    for b in range(n_blk):
        pltpu.make_async_copy(x_scr.at[blk_rows(b)], y_hbm.at[blk_rows(b)], io_sem.at[b]).wait()


def run_layers(mesh, x_act, lens, w_in, w_out, w_kv, gain, t_loc):
    n_tok, d_model = x_act.shape
    n_layers, f_loc, in_loc = w_in.shape
    out_loc = w_out.shape[1]
    n_y, n_model = mesh.shape["data"], mesh.shape["model"]
    n_x = n_model // CORES
    head_dim = w_kv.shape[2] // 2
    n_seqs = n_tok // t_loc
    s_len = t_loc * n_model
    rows_blk = SEQS_BLOCK * t_loc
    n_blk = n_tok // rows_blk
    sizes = {("kv", 0): SEQS_BLOCK * t_loc * 4 * head_dim}
    for k, (n_rows, n_cols, split) in enumerate(((f_loc, in_loc, IN_SPLIT), (out_loc, f_loc, OUT_SPLIT))):
        row = 2 * n_cols
        sizes |= {("lo", k): split * row, ("lo4", k): n_y * split * row, ("hi", k): (n_rows - split) * row, ("all", k): n_y * n_rows * row}
    keys, plan, _ = make_plan(n_layers, n_x, n_blk, sizes)
    n_sem = len(keys) + 2 * (n_y - 1)
    cfg = {"dims": (n_layers, n_y, n_x, t_loc, s_len, head_dim, in_loc, out_loc, n_seqs), "plan": (keys, plan)}
    vmem = pl.BlockSpec(memory_space=pltpu.VMEM)
    hbm = pl.BlockSpec(memory_space=pl.ANY)
    gain8 = jnp.broadcast_to(gain.astype(F32)[:, None, :], (n_layers, 8, f_loc))
    return pl.pallas_call(
        functools.partial(kernel_body, cfg),
        out_shape=(
            jax.ShapeDtypeStruct((n_tok, d_model), BF16),
            jax.ShapeDtypeStruct((n_layers, CORES, n_x, n_y, f_loc, in_loc), BF16),
            jax.ShapeDtypeStruct((n_layers, CORES, n_x, n_y, out_loc, f_loc), BF16),
        ),
        in_specs=[pl.BlockSpec(memory_space=pltpu.SMEM), hbm, hbm, hbm, vmem, vmem],
        out_specs=(hbm, hbm, hbm),
        scratch_shapes=[
            pltpu.VMEM((2, n_y, f_loc, CORES * in_loc), BF16),
            pltpu.VMEM((2, n_y, CORES * out_loc, f_loc), BF16),
            pltpu.VMEM((n_layers, n_seqs, s_len, 2 * head_dim), BF16),
            pltpu.VMEM((n_layers, n_y, f_loc, 2 * head_dim), BF16),
            pltpu.VMEM((n_layers, n_y, 8, f_loc), F32),
            pltpu.VMEM((n_tok, d_model), BF16),
            pltpu.VMEM((n_tok, d_model), BF16),
            pltpu.VMEM((n_tok, d_model), F32),
            pltpu.VMEM((rows_blk, CORES * in_loc), BF16),
            pltpu.VMEM((rows_blk, CORES * out_loc), BF16),
            pltpu.VMEM((2 * CORES * t_loc, s_len), F32),
            pltpu.VMEM((2 * CORES * t_loc, s_len), F32),
            pltpu.VMEM((2 * CORES * t_loc, s_len), BF16),
            pltpu.VMEM((2 * CORES * t_loc, s_len), BF16),
            pltpu.SemaphoreType.DMA((n_sem,)),
            pltpu.SemaphoreType.DMA((n_sem,)),
            pltpu.SemaphoreType.DMA((2, 4)),
            pltpu.SemaphoreType.DMA((n_blk,)),
            pltpu.SemaphoreType.DMA((n_layers, 2)),
        ],
        compiler_params=pltpu.CompilerParams(collective_id=0, has_side_effects=True, vmem_limit_bytes=67043328 - 1024 * 1024),
        name="layers",
    )(lens, x_act, w_in, w_out, w_kv, gain8)[0]


def solution(mesh):
    act_spec = P(None, ("part", "data"), "model", None)

    def local_fn(x_blk, len_blk, gain_blk, w_in_blk, w_kv_blk, w_out_blk):
        n_micro, n_seqs, t_loc, d_model = x_blk.shape
        x_act = x_blk.reshape(n_micro * n_seqs * t_loc, d_model)
        y = run_layers(mesh, x_act, len_blk.reshape(-1), w_in_blk, w_out_blk, w_kv_blk, gain_blk, t_loc)
        return y.reshape(x_blk.shape)

    return jax.shard_map(
        local_fn,
        mesh=mesh,
        in_specs=(act_spec, P(None, ("part", "data")), P(None, "data"), P(None, "data", "model"), P(None, "data", None), P(None, "model", "data")),
        out_specs=act_spec,
        check_vma=False,
    )
```
